128 devices in a mesh: grp: 4 (over z_lo, core), dp: 32 (over z_hi, y, x).
Axes of the slice: x: 4, y: 4, z: 4 (z_hi: 2, z_lo: 2; z = z_hi * 2 + z_lo), core: 2. Of those that a mesh axis runs over, the one named last changes fastest.
Arguments:
- activations: bfloat16 [262144, 1280], P(('grp', 'dp')), may hold values from -6 to 6
- cotangent: bfloat16 [262144, 1280], P(('grp', 'dp')), may hold values from -0.01171875 to 0.01171875
- carried_error: float32 [128, 1280, 1280], P(('grp', 'dp')), may hold values from -6 to 6
- owner_error: float32 [1280, 1280], P(('grp', 'dp')), may hold values from -6 to 6
Outputs:
- update: float32 [1280, 1280], replicated
The draws below stay inside these ranges and needn't reach their ends.
All inputs are finite; a program needn't handle non-finite values.
Results may differ from the reference program's by a relative error of at most 0.012.
Values may be sent and summed in bfloat16 or wider, within the bound.
No kernel may reach another device: no remote copies, remote signals or barrier semaphores. Data moves between devices by JAX's collectives and lax.ppermute only.
A program may use at most 128 MiB of HBM per device.

```python
import jax
import jax.numpy as jnp
from jax import lax

D = 1280
BLOCK = 128
TOK_DEV = 2048
TOKENS = 262144
N_GRP = 4
N_DP = 32
DEVICES = 128


def strengthened(entries, stream_key, source, target, shards_of, factor):
    owner, partner = [(jnp.arange(entries.shape[position]) // (entries.shape[position] // shards_of)).reshape([-1 if axis == position else 1 for axis in range(entries.ndim)]) for position in (source, target)]
    chosen = jax.random.permutation(stream_key, shards_of)[partner]
    strong = (owner == chosen) | (owner == (partner + shards_of // 2) % shards_of)
    return jnp.where(strong, factor * entries, entries)


def shard_levels(own_key, shape, split, low, top_value):
    def one(axis_at, blocks):
        heights = jax.random.uniform(jax.random.fold_in(jax.random.fold_in(own_key, 6), axis_at), (blocks,), jnp.float32, low / len(split), top_value / len(split))
        return jnp.repeat(jnp.exp(heights), shape[axis_at] // blocks).reshape((-1,) + (1,) * (len(shape) - axis_at - 1))

    factor_of = one(*split[0])
    for cut in split[1:]:
        factor_of = factor_of * one(*cut)
    return factor_of


def bell_draw(stream_key, dims, spread, bound, cuts=(), kind=jnp.bfloat16):
    level = shard_levels(stream_key, dims, cuts, -0.22, 0.18) if cuts else 1.0
    values = jax.random.normal(stream_key, dims, jnp.float32) * spread * level
    return jnp.minimum(jnp.maximum(values, -bound), bound).astype(kind)


def gaussian_with(stream_key, dims, deviation, bound, shards, heavy, kind=jnp.bfloat16):
    values = deviation * jax.random.normal(stream_key, dims, jnp.float32)
    if shards:
        values = values * shard_levels(stream_key, dims, shards, -0.22, 0.18)
    return jnp.clip(strengthened(values, jax.random.fold_in(stream_key, 3), *heavy), -bound, bound).astype(kind)


def setup_inputs(seed: int = 0) -> dict:
    key_of = jax.random.split(jax.random.key(seed), 5)
    return {
        "activations": bell_draw(key_of[0], (TOKENS, D), 1.0, 6.0, ((0, 128),)),
        "cotangent": bell_draw(key_of[1], (TOKENS, D), (TOK_DEV * N_GRP * N_DP) ** -0.5, 0.01171875, ((0, 128),)),
        "carried_error": gaussian_with(key_of[2], (DEVICES, D, D), 0.1, 6.0, ((0, 128),), (0, 1, 128, 5.5), jnp.float32),
        "owner_error": bell_draw(key_of[3], (D, D), 0.5, 6.0, ((0, 128),), jnp.float32),
    }


def quantize(values):
    blocks = values.reshape(values.shape[:-1] + (values.shape[-1] // BLOCK, BLOCK))
    largest = jnp.max(jnp.abs(blocks), axis=-1)
    scales = ((largest + 1e-6) / 127.0).astype(jnp.bfloat16)
    levels = (blocks / scales.astype(jnp.float32)[..., None]).astype(jnp.bfloat16)
    return levels.reshape(values.shape), scales


def dequantize(levels, scales):
    blocks = levels.reshape(levels.shape[:-1] + (levels.shape[-1] // BLOCK, BLOCK)).astype(jnp.float32)
    return (blocks * scales.astype(jnp.float32)[..., None]).reshape(levels.shape)


def reference(activations, cotangent, carried_error, owner_error):
    inputs_dev = activations.reshape(DEVICES, TOK_DEV, D)
    grads_dev = cotangent.reshape(DEVICES, TOK_DEV, D)

    def add_device(summed, pieces):
        inputs_one, grads_one, error_one = pieces
        gradient = lax.dot_general(inputs_one.astype(jnp.float32), grads_one.astype(jnp.float32), (((0,), (0,)), ((), ())), preferred_element_type=jnp.float32)
        levels, scales = quantize(gradient + error_one)
        return summed + dequantize(levels, scales), None

    summed, unused = lax.scan(add_device, jnp.zeros((D, D), jnp.float32), (inputs_dev, grads_dev, carried_error))
    summed = summed + owner_error
    owner_level, owner_scale = quantize(summed)
    return dequantize(owner_level, owner_scale)
```

```python
import functools

import jax
import jax.numpy as jnp
from jax import lax
from jax.experimental import pallas as pl
from jax.experimental.pallas import tpu as pltpu
from jax.sharding import Mesh
from jax.sharding import PartitionSpec as P

D = 1280
BLOCK = 128
HALF = D // 2
COLS = D // BLOCK
AXES = ("zl", "c", "zh", "y", "x")
CHIPS = ("zl", "zh", "y", "x")
N_CHIPS = 64
TILES = HALF // 8 * COLS
PER_CHIP = -(-TILES // N_CHIPS)
OWNED = PER_CHIP * 8
STEP = 128


def quantized(v):
    largest = jnp.max(jnp.abs(v), axis=-1, keepdims=True)
    scale = ((largest + 1e-06) / 127.0).astype(jnp.bfloat16).astype(jnp.float32)
    level = (v * (1.0 / scale)).astype(jnp.bfloat16).astype(jnp.float32)
    return level * scale


def gradient_kernel(where, act, cot, err, window, out, acc):
    acc[...] = lax.dot_general(
        act[...], cot[...], (((0,), (0,)), ((), ())), preferred_element_type=jnp.float32
    )
    for b in range(COLS):
        at = slice(b * BLOCK, (b + 1) * BLOCK)
        acc[:, at] = quantized(acc[:, at] + err[:, at])
    first = (where[0] + pl.program_id(0)) * STEP
    for k in range(2):
        row = where[1] + 8 * k - first

        @pl.when((row >= 0) & (row < STEP))
        def _():
            rows = pl.ds(pl.multiple_of(row, 8), 8)
            acc[rows, :] = acc[rows, :] + window[8 * k : 8 * k + 8, :]

    out[...] = acc[...].astype(out.dtype)


def half_gradient(where, act, cot, err, window, dtype, name):
    tokens = act.shape[0]
    return pl.pallas_call(
        gradient_kernel,
        out_shape=jax.ShapeDtypeStruct((HALF, D), dtype),
        grid_spec=pltpu.PrefetchScalarGridSpec(
            num_scalar_prefetch=1,
            grid=(HALF // STEP,),
            in_specs=[
                pl.BlockSpec((tokens, STEP), lambda i, w: (0, w[0] + i)),
                pl.BlockSpec((tokens, D), lambda i, w: (0, 0)),
                pl.BlockSpec((STEP, D), lambda i, w: (w[0] + i, 0)),
                pl.BlockSpec((16, D), lambda i, w: (0, 0)),
            ],
            out_specs=pl.BlockSpec((STEP, D), lambda i, w: (i, 0)),
            scratch_shapes=[pltpu.VMEM((STEP, D), jnp.float32)],
        ),
        cost_estimate=pl.CostEstimate(
            flops=2 * tokens * HALF * D, bytes_accessed=12 << 20, transcendentals=0
        ),
        name=name,
    )(where, act, cot, err, window)


def pair_kernel(own, got, out):
    for b in range(COLS):
        at = slice(b * BLOCK, (b + 1) * BLOCK)
        both = own[:, at] + got[:, at].astype(jnp.float32)
        out[:, b] = both.astype(jnp.bfloat16).reshape(-1, 8, BLOCK)


def pair_sum(own, got):
    out = pl.pallas_call(
        pair_kernel,
        out_shape=jax.ShapeDtypeStruct((N_CHIPS * PER_CHIP // COLS + 1, COLS, 8, BLOCK), jnp.bfloat16),
        grid=(HALF // STEP,),
        in_specs=[
            pl.BlockSpec((STEP, D), lambda i: (i, 0)),
            pl.BlockSpec((STEP, D), lambda i: (i, 0)),
        ],
        out_specs=pl.BlockSpec((STEP // 8, COLS, 8, BLOCK), lambda i: (i, 0, 0, 0)),
        cost_estimate=pl.CostEstimate(flops=HALF * D, bytes_accessed=7 << 20, transcendentals=0),
        name="pair",
    )(own, got)
    return out


def owner_kernel(parts, out):
    total = jnp.sum(parts[...].astype(jnp.float32), axis=0)
    update = quantized(total).astype(jnp.bfloat16)
    for k in range(N_CHIPS):
        out[k] = update


def owner_update(parts):
    return pl.pallas_call(
        owner_kernel,
        out_shape=jax.ShapeDtypeStruct((N_CHIPS, OWNED, BLOCK), jnp.bfloat16),
        in_specs=[pl.BlockSpec(memory_space=pltpu.VMEM)],
        out_specs=pl.BlockSpec(memory_space=pltpu.VMEM),
        cost_estimate=pl.CostEstimate(
            flops=N_CHIPS * OWNED * BLOCK, bytes_accessed=4 << 20, transcendentals=0
        ),
        name="owner",
    )(parts)


def widen_kernel(where, part, *rest):
    out = rest[-1]
    for b in range(COLS):
        out[:, b * BLOCK : (b + 1) * BLOCK] = (
            part[:, b].astype(jnp.float32).reshape(-1, BLOCK)
        )


def widen(where, part, base, name):
    specs = [pl.BlockSpec((STEP // 8, COLS, 8, BLOCK), lambda i, w: (i, 0, 0, 0))]
    args = [where, part]
    aliases = {}
    if base is not None:
        specs.append(pl.BlockSpec(memory_space=pl.ANY))
        args.append(base)
        aliases = {2: 0}
    return pl.pallas_call(
        widen_kernel,
        out_shape=jax.ShapeDtypeStruct((D, D), jnp.float32),
        grid_spec=pltpu.PrefetchScalarGridSpec(
            num_scalar_prefetch=1,
            grid=(HALF // STEP,),
            in_specs=specs,
            out_specs=pl.BlockSpec((STEP, D), lambda i, w: (w[0] + i, 0)),
        ),
        input_output_aliases=aliases,
        cost_estimate=pl.CostEstimate(flops=HALF * D, bytes_accessed=5 << 20, transcendentals=0),
        name=name,
    )(*args)


def swap_cores(value):
    return lax.ppermute(value, "c", [(0, 1), (1, 0)])


def on_device(activations, cotangent, carried_error, owner_error):
    core = lax.axis_index("c")
    rows = owner_error.shape[0]
    first = lax.axis_index(AXES) * rows
    aligned = first // 8 * 8
    window = lax.dynamic_update_slice(
        jnp.zeros((16, D), jnp.float32), owner_error, (first - aligned, 0)
    )
    steps = HALF // STEP
    mine = jnp.stack([core * steps, aligned]).astype(jnp.int32)
    theirs = jnp.stack([(1 - core) * steps, aligned]).astype(jnp.int32)
    error = carried_error.reshape(D, D)
    to_send = half_gradient(theirs, activations, cotangent, error, window, jnp.bfloat16, "send_half")
    got = swap_cores(to_send)
    own = half_gradient(mine, activations, cotangent, error, window, jnp.float32, "own_half")
    sums = pair_sum(own, got)
    sums = sums.reshape(-1, 8, BLOCK)[: N_CHIPS * PER_CHIP].reshape(N_CHIPS, OWNED, BLOCK)
    parts = lax.all_to_all(sums, CHIPS, 0, 0, tiled=True)
    update = owner_update(parts)
    all_mine = lax.all_to_all(update, CHIPS, 0, 0, tiled=True)
    all_mine = all_mine.reshape(-1, 8, BLOCK)[:TILES].reshape(HALF // 8, COLS, 8, BLOCK)
    all_theirs = swap_cores(all_mine)
    half_out = widen(mine[:1], all_mine, None, "widen_own")
    return widen(theirs[:1], all_theirs, half_out, "widen_other")


def solution(mesh):
    fine = Mesh(mesh.devices.reshape(2, 2, 2, 4, 4), AXES)
    return jax.shard_map(
        on_device,
        mesh=fine,
        in_specs=(P(AXES, None), P(AXES, None), P(AXES, None, None), P(AXES, None)),
        out_specs=P(),
        check_vma=False,
    )
```

```python
import jax
import jax.numpy as jnp
import numpy as np
from jax import lax
from jax.experimental import pallas as pl
from jax.experimental.pallas import tpu as pltpu
from jax.sharding import Mesh
from jax.sharding import PartitionSpec as P


D = 1280
BLOCK = 128
HALF = D // 2
COLS = D // BLOCK
AXES = ("zl", "c", "zh", "y", "x")
SIZES = (2, 2, 2, 4, 4)
QUARTER = HALF // 4
TILES = QUARTER // 8 * COLS
PER_CHIP = -(-TILES // 16)
OWNED = PER_CHIP * 8
CHUNK = 512
ORDER = (2, 1, 3, 0)
MIB = 1 << 20
GRANT = 46


def device(zl, c, zh, y, x):
    return int(np.ravel_multi_index((zl, c, zh, y, x), SIZES))


def line(core, lead):
    spots = [(zl, zh, o) for zl in range(2) for zh in range(2) for o in range(4)]
    if core == 0:
        return [device(zl, 0, zh, o, lead) for zl, zh, o in spots]
    return [device(zl, 1, zh, lead, o) for zl, zh, o in spots]


SIXTEENS = [line(core, lead) for core in range(2) for lead in range(4)]


def from_ahead(k):
    pairs = []
    for core in range(2):
        for lead in range(4):
            pairs += list(zip(line(core, (lead + k) % 4), line(core, lead)))
    return pairs


def to_ahead(k):
    return [(source, target) for target, source in from_ahead(k)]


def params(mib, **more):
    return pltpu.CompilerParams(vmem_limit_bytes=mib * MIB, **more)


def quantized(v):
    largest = jnp.max(jnp.abs(v), axis=-1, keepdims=True)
    scale = ((largest + 1e-06) / 127.0).astype(jnp.bfloat16).astype(jnp.float32)
    level = (v * (1.0 / scale)).astype(jnp.bfloat16).astype(jnp.float32)
    return level * scale


def multiplied(a, c):
    return lax.dot_general(a, c, (((0,), (0,)), ((), ())), preferred_element_type=jnp.float32)


def gradient_kernel(places, spot, act, cot, error, owner, sent, kept, acc, err, sem):
    load = pltpu.make_async_copy(error, err, sem)

    def step(a, c):
        first = pl.program_id(0) == 0

        @pl.when(first)
        def _():
            load.start()
            for m in range(0, D, 256):
                acc[m : m + 256, :] = multiplied(a[:, m : m + 256], c[...])

        @pl.when(jnp.logical_not(first))
        def _():
            for m in range(0, D, 256):
                acc[m : m + 256, :] = acc[m : m + 256, :] + multiplied(a[:, m : m + 256], c[...])

    pltpu.emit_pipeline(
        step,
        grid=(act.shape[0] // CHUNK,),
        in_specs=[
            pl.BlockSpec((CHUNK, D), lambda i: (i, 0)),
            pl.BlockSpec((CHUNK, D), lambda i: (i, 0)),
        ],
    )(act, cot)
    load.wait()
    row = spot[0]
    aligned = row // 8 * 8
    for half, out in enumerate((sent, kept)):

        @pl.loop(0, 4)
        def _(k):
            start = pl.multiple_of(places[half] + (places[2 + half] + k) % 4 * QUARTER, 32)
            rows = pl.ds(start, QUARTER)
            for b in range(COLS):
                at = slice(b * BLOCK, (b + 1) * BLOCK)
                block = quantized(acc[rows, at] + err[rows, at])
                acc[rows, at] = block
                out[k, :, at] = block.astype(out.dtype)

        @pl.loop(0, 2)
        def _(i):
            tile = aligned + 8 * i
            inside = tile - places[half]

            @pl.when((inside >= 0) & (inside < HALF))
            def _():
                k = (inside // QUARTER + 4 - places[2 + half]) % 4
                add_owner(acc, owner, out, tile, row, k, inside % QUARTER)


def add_owner(acc, owner, out, tile, row, k, at):
    for shift in (-8, -6, -4, -2, 0, 2, 4, 6):

        @pl.when(row - tile == shift)
        def _():
            low, high = max(shift, 0), min(shift + 10, 8)
            mine = owner[low - shift : high - shift, :]
            mine = jnp.pad(mine, ((low, 8 - high), (0, 0)))
            total = acc[pl.ds(pl.multiple_of(tile, 8), 8), :] + mine
            out[k, pl.ds(pl.multiple_of(at, 8), 8), :] = total.astype(out.dtype)


def gradient(places, spot, act, cot, error, owner):
    return pl.pallas_call(
        gradient_kernel,
        out_shape=(
            jax.ShapeDtypeStruct((4, QUARTER, D), jnp.bfloat16),
            jax.ShapeDtypeStruct((4, QUARTER, D), jnp.float32),
        ),
        in_specs=[pl.BlockSpec(memory_space=pltpu.SMEM)] * 2
        + [pl.BlockSpec(memory_space=pltpu.HBM)] * 3
        + [pl.BlockSpec(memory_space=pltpu.VMEM)],
        out_specs=(pl.BlockSpec(memory_space=pltpu.VMEM),) * 2,
        scratch_shapes=[
            pltpu.VMEM((D, D), jnp.float32),
            pltpu.VMEM((D, D), jnp.float32),
            pltpu.SemaphoreType.DMA,
        ],
        compiler_params=params(GRANT),
        cost_estimate=pl.CostEstimate(
            flops=2 * act.shape[0] * D * D, bytes_accessed=17 * MIB, transcendentals=0
        ),
        name="gradient",
    )(places, spot, act, cot, error, owner)


def pair_kernel(kept, got, out):
    out[...] = (kept[0] + got[...].astype(jnp.float32)).astype(out.dtype)


def pair(kept, got, k, dtype):
    return pl.pallas_call(
        pair_kernel,
        out_shape=jax.ShapeDtypeStruct((QUARTER, D), dtype),
        grid=(1,),
        in_specs=[
            pl.BlockSpec((1, QUARTER, D), lambda i: (k, 0, 0)),
            pl.BlockSpec((QUARTER, D), lambda i: (0, 0)),
        ],
        out_specs=pl.BlockSpec((QUARTER, D), lambda i: (0, 0)),
        compiler_params=params(6),
        cost_estimate=pl.CostEstimate(flops=1 << 28, bytes_accessed=2 * MIB, transcendentals=0),
    )(kept, got)


def total_kernel(own, *rest):
    out = rest[-1]
    for b in range(COLS):
        at = slice(b * BLOCK, (b + 1) * BLOCK)
        total = own[:, at]
        for got in rest[:-1]:
            total = total + got[:, at].astype(jnp.float32)
        total = total.astype(jnp.bfloat16).reshape(QUARTER // 8, 8, BLOCK)
        for r in range(QUARTER // 8):
            out[r * COLS + b] = total[r]
    out[TILES:] = jnp.zeros_like(out[TILES:])


def total_of(own, others):
    return pl.pallas_call(
        total_kernel,
        out_shape=jax.ShapeDtypeStruct((16 * PER_CHIP, 8, BLOCK), jnp.bfloat16),
        in_specs=[pl.BlockSpec(memory_space=pltpu.VMEM)] * (1 + len(others)),
        out_specs=pl.BlockSpec(memory_space=pltpu.VMEM),
        compiler_params=params(4),
        cost_estimate=pl.CostEstimate(flops=4 * QUARTER * D, bytes_accessed=2 * MIB, transcendentals=0),
        name="total",
    )(own, *others)


def owner_kernel(parts, out):
    total = parts[0].astype(jnp.float32)
    for k in range(1, parts.shape[0]):
        total = total + parts[k].astype(jnp.float32)
    update = quantized(total).astype(jnp.bfloat16)
    for k in range(out.shape[0]):
        out[k] = update


def owner_update(parts):
    return pl.pallas_call(
        owner_kernel,
        out_shape=jax.ShapeDtypeStruct((16, OWNED, BLOCK), jnp.bfloat16),
        in_specs=[pl.BlockSpec(memory_space=pltpu.VMEM)],
        out_specs=pl.BlockSpec(memory_space=pltpu.VMEM),
        compiler_params=params(8),
        cost_estimate=pl.CostEstimate(
            flops=parts.size, bytes_accessed=2 * MIB, transcendentals=0
        ),
        name="owner",
    )(parts)


def widen_kernel(where, part, *rest):
    out = rest[-1]
    for r in range(QUARTER // 8):
        for b in range(COLS):
            out[r * 8 : r * 8 + 8, b * BLOCK : (b + 1) * BLOCK] = part[r * COLS + b].astype(
                jnp.float32
            )


def widen(where, part, base):
    specs = [pl.BlockSpec((TILES, 8, BLOCK), lambda i, w: (0, 0, 0))]
    args = [where, part]
    aliases = {}
    if base is not None:
        specs.append(pl.BlockSpec(memory_space=pl.ANY))
        args.append(base)
        aliases = {2: 0}
    return pl.pallas_call(
        widen_kernel,
        out_shape=jax.ShapeDtypeStruct((D, D), jnp.float32),
        grid_spec=pltpu.PrefetchScalarGridSpec(
            num_scalar_prefetch=1,
            grid=(1,),
            in_specs=specs,
            out_specs=pl.BlockSpec((QUARTER, D), lambda i, w: (w[0], 0)),
        ),
        input_output_aliases=aliases,
        compiler_params=params(4),
        cost_estimate=pl.CostEstimate(
            flops=1 << 30, bytes_accessed=MIB, transcendentals=0
        ),
        name="widen",
    )(*args)


def swap_cores(value):
    return lax.ppermute(value, "c", [(0, 1), (1, 0)])


def one(value):
    return value.astype(jnp.int32).reshape(1)


def on_device(activations, cotangent, carried_error, owner_error):
    core = lax.axis_index("c")
    x, y = lax.axis_index("x"), lax.axis_index("y")
    lead = jnp.where(core == 0, x, y)
    other_lead = x + y - lead
    spot = one(lax.axis_index(AXES) * owner_error.shape[0])
    error = carried_error.reshape(D, D)
    places = jnp.stack([(1 - core) * HALF, core * HALF, other_lead, lead]).astype(jnp.int32)
    sent, kept = gradient(places, spot, activations, cotangent, error, owner_error)
    got = {}
    for k in ORDER:
        got[k] = swap_cores(sent[k])
    arrived = []
    for k in ORDER:
        whole = k == 0
        piece = pair(kept, got[k], k, jnp.float32 if whole else jnp.bfloat16)
        if whole:
            own = piece
        else:
            arrived.append(lax.ppermute(piece, AXES, to_ahead(k)))
    parts = total_of(own, arrived).reshape(16, OWNED, BLOCK)
    parts = lax.all_to_all(parts, AXES, 0, 0, axis_index_groups=SIXTEENS, tiled=True)
    update = owner_update(parts)
    mine = lax.all_to_all(update, AXES, 0, 0, axis_index_groups=SIXTEENS, tiled=True)
    mine = mine.reshape(16 * PER_CHIP, 8, BLOCK)[:TILES]
    pieces = [(0, mine)]
    for k in (2, 1, 3):
        pieces.append((k, lax.ppermute(mine, AXES, from_ahead(k))))
    out = None
    for k, piece in pieces:
        if out is not None:
            piece, out = lax.optimization_barrier((piece, out))
        other = swap_cores(piece)
        out = widen(one(core * 4 + (lead + k) % 4), piece, out)
        out = widen(one((1 - core) * 4 + (other_lead + k) % 4), other, out)
    return out


def solution(mesh):
    fine = Mesh(mesh.devices.reshape(SIZES), AXES)
    return jax.shard_map(
        on_device,
        mesh=fine,
        in_specs=(P(AXES, None), P(AXES, None), P(AXES, None, None), P(AXES, None)),
        out_specs=P(),
        check_vma=False,
    )
```

```python
import functools

import jax
import jax.numpy as jnp
import numpy as np
from jax import lax
from jax.experimental import pallas as pl
from jax.experimental.pallas import tpu as pltpu
from jax.sharding import Mesh
from jax.sharding import PartitionSpec as P


D = 1280
BLOCK = 128
HALF = D // 2
COLS = D // BLOCK
AXES = ("zl", "c", "zh", "y", "x")
SIZES = (2, 2, 2, 4, 4)
QUARTER = HALF // 4
TILES = QUARTER // 8 * COLS
PER_CHIP = -(-TILES // 16)
OWNED = PER_CHIP * 8
CHUNK = 512
MROWS = 256
EARLY = 3
WSTEPS = 5
MIB = 1 << 20
GRANT = 34
ORDER = (2, 1, 3, 0)
WRITES = {
    "write_0": ((0, True), (0, False)),
    "write_1": ((1, True), (1, False)),
    "write_2": ((3, True),),
    "write_3": ((3, False), (2, True)),
    "write_4": ((2, False),),
}


def device(zl, c, zh, y, x):
    return int(np.ravel_multi_index((zl, c, zh, y, x), SIZES))


def line(core, lead):
    spots = [(zl, zh, o) for zl in range(2) for zh in range(2) for o in range(4)]
    if core == 0:
        return [device(zl, 0, zh, o, lead) for zl, zh, o in spots]
    return [device(zl, 1, zh, lead, o) for zl, zh, o in spots]


SIXTEENS = [line(core, lead) for core in range(2) for lead in range(4)]


def from_ahead(k):
    pairs = []
    for core in range(2):
        for lead in range(4):
            pairs += list(zip(line(core, (lead + k) % 4), line(core, lead)))
    return pairs


def to_ahead(k):
    return [(source, target) for target, source in from_ahead(k)]


def params(mib, **more):
    return pltpu.CompilerParams(vmem_limit_bytes=mib * MIB, **more)


def quantized(v):
    largest = jnp.max(jnp.abs(v), axis=-1, keepdims=True)
    scale = ((largest + 1e-06) / 127.0).astype(jnp.bfloat16).astype(jnp.float32)
    level = (v * (1.0 / scale)).astype(jnp.bfloat16).astype(jnp.float32)
    return level * scale


def piece_start(core, quarter):
    return quarter // 2 * HALF + core * (HALF // 2) + quarter % 2 * QUARTER


def piece_index(core, quarter):
    return quarter // 2 * 4 + core * 2 + quarter % 2


def multiplied(a, c):
    return lax.dot_general(a, c, (((0,), (0,)), ((), ())), preferred_element_type=jnp.float32)


def gradient_kernel(
    spot, act, cot, error, owner, v, early_v, late_v, cot_v, err, own, acc, early_sem, late_sem, cot_sem, err_sem, own_sem
):
    chunks = cot.shape[0] // CHUNK
    blocks = D // MROWS

    def slab(i):
        return pl.ds(i * CHUNK, CHUNK)

    def early(i):
        return (
            pltpu.make_async_copy(
                act.at[slab(i), pl.ds(0, EARLY * MROWS)], early_v.at[slab(i), :], early_sem.at[i]
            ),
            pltpu.make_async_copy(cot.at[slab(i), :], cot_v.at[slab(i), :], cot_sem.at[i]),
        )

    def late(j):
        return pltpu.make_async_copy(
            act.at[:, pl.ds(j * MROWS, MROWS)], late_v.at[j - EARLY], late_sem.at[j - EARLY]
        )

    def load_err(j):
        at = pl.ds(j * MROWS, MROWS)
        return pltpu.make_async_copy(error.at[at, :], err.at[at, :], err_sem.at[j])

    def finish(j):
        at = slice(j * MROWS, (j + 1) * MROWS)
        for b in range(0, D, BLOCK):
            cols = slice(b, b + BLOCK)
            v[at, cols] = quantized(acc[at, cols] + err[at, cols])

    load_own = pltpu.make_async_copy(owner, own, own_sem)
    for i in range(2):
        for copy in early(i):
            copy.start()
    for i in range(chunks):
        for copy in early(i):
            copy.wait()
        if i + 2 < chunks:
            for copy in early(i + 2):
                copy.start()
        elif i + 2 == chunks:
            late(EARLY).start()
            for j in range(blocks):
                load_err(j).start()
                if EARLY < j + EARLY + 1 < blocks:
                    late(j + EARLY + 1).start()
            load_own.start()
        for j in range(EARLY):
            at = slice(j * MROWS, (j + 1) * MROWS)
            product = multiplied(early_v[i * CHUNK : (i + 1) * CHUNK, at], cot_v[i * CHUNK : (i + 1) * CHUNK, :])
            acc[at, :] = product if i == 0 else acc[at, :] + product
    done = 0
    for j in range(EARLY, blocks):
        late(j).wait()
        ready = j if j + 1 == blocks else min(j, done + 2 if j > EARLY else 1)
        for q in range(done, ready):
            load_err(q).wait()
        acc[j * MROWS : (j + 1) * MROWS, :] = multiplied(late_v[j - EARLY], cot_v[...])
        for q in range(done, ready):
            finish(q)
        done = ready
    load_own.wait()
    for q in range(done, blocks):
        load_err(q).wait()
        finish(q)
    row = spot[0]
    for shift in (0, 2, 4, 6):

        @pl.when(row % 8 == shift)
        def _():
            for i in range(2):
                low, high = max(shift - 8 * i, 0), min(shift + 10 - 8 * i, 8)
                rows = pl.ds(pl.multiple_of(row // 8 * 8 + 8 * i, 8), 8)
                mine = own[low - shift + 8 * i : high - shift + 8 * i, :]
                v[rows, :] = v[rows, :] + jnp.pad(mine, ((low, 8 - high), (0, 0)))


def gradient(spot, act, cot, error, owner):
    tokens = act.shape[0]
    hbm, vmem = pl.BlockSpec(memory_space=pltpu.HBM), pl.BlockSpec(memory_space=pltpu.VMEM)
    blocks, chunks = D // MROWS, tokens // CHUNK
    return pl.pallas_call(
        gradient_kernel,
        out_shape=pltpu.VMEM((D, D), jnp.float32),
        in_specs=[pl.BlockSpec(memory_space=pltpu.SMEM)] + [hbm] * 4,
        out_specs=vmem,
        scratch_shapes=[
            pltpu.VMEM((tokens, EARLY * MROWS), jnp.bfloat16),
            pltpu.VMEM((blocks - EARLY, tokens, MROWS), jnp.bfloat16),
            pltpu.VMEM((tokens, D), jnp.bfloat16),
            pltpu.VMEM((D, D), jnp.float32),
            pltpu.VMEM(owner.shape, jnp.float32),
            pltpu.VMEM((D, D), jnp.float32),
            pltpu.SemaphoreType.DMA((chunks,)),
            pltpu.SemaphoreType.DMA((blocks - EARLY,)),
            pltpu.SemaphoreType.DMA((chunks,)),
            pltpu.SemaphoreType.DMA((blocks,)),
            pltpu.SemaphoreType.DMA,
        ],
        compiler_params=params(GRANT),
        cost_estimate=pl.CostEstimate(
            flops=2 * tokens * D * D, bytes_accessed=17 * MIB, transcendentals=0
        ),
        name="gradient",
    )(spot, act, cot, error, owner)


def multiplied(a, c):
    return lax.dot_general(a, c, (((0,), (0,)), ((), ())), preferred_element_type=jnp.float32)


def pick_kernel(core, lead, v, *outs):
    for k, out in enumerate(outs):
        start = piece_start(core[0], (lead[0] + k) % 4)
        out[...] = v[pl.ds(pl.multiple_of(start, 32), QUARTER), :].astype(out.dtype)


def pick(core, lead, v):
    smem, vmem = pl.BlockSpec(memory_space=pltpu.SMEM), pl.BlockSpec(memory_space=pltpu.VMEM)
    return pl.pallas_call(
        pick_kernel,
        out_shape=[jax.ShapeDtypeStruct((QUARTER, D), jnp.bfloat16)] * 4,
        in_specs=[smem, smem, vmem],
        out_specs=[vmem] * 4,
        compiler_params=params(4),
        cost_estimate=pl.CostEstimate(flops=1 << 28, bytes_accessed=2 * MIB, transcendentals=0),
        name="pick",
    )(core, lead, v)


def pair_kernel(k, core, lead, v, got, out):
    start = piece_start(core[0], (lead[0] + k) % 4)
    kept = v[pl.ds(pl.multiple_of(start, 32), QUARTER), :]
    out[...] = (kept + got[...].astype(jnp.float32)).astype(out.dtype)


def pair(core, lead, v, got, k):
    smem, vmem = pl.BlockSpec(memory_space=pltpu.SMEM), pl.BlockSpec(memory_space=pltpu.VMEM)
    return pl.pallas_call(
        functools.partial(pair_kernel, k),
        out_shape=jax.ShapeDtypeStruct((QUARTER, D), jnp.bfloat16 if k else jnp.float32),
        in_specs=[smem, smem, vmem, vmem],
        out_specs=vmem,
        compiler_params=params(4),
        cost_estimate=pl.CostEstimate(flops=1 << 28, bytes_accessed=2 * MIB, transcendentals=0),
    )(core, lead, v, got)


def total_kernel(own, *rest):
    out = rest[-1]
    for b in range(COLS):
        at = slice(b * BLOCK, (b + 1) * BLOCK)
        total = own[:, at]
        for got in rest[:-1]:
            total = total + got[:, at].astype(jnp.float32)
        total = total.astype(jnp.bfloat16).reshape(QUARTER // 8, 8, BLOCK)
        for r in range(QUARTER // 8):
            out[r * COLS + b] = total[r]
    out[TILES:] = jnp.zeros_like(out[TILES:])


def total_of(own, *others):
    return pl.pallas_call(
        total_kernel,
        out_shape=jax.ShapeDtypeStruct((16 * PER_CHIP, 8, BLOCK), jnp.bfloat16),
        in_specs=[pl.BlockSpec(memory_space=pltpu.VMEM)] * (1 + len(others)),
        out_specs=pl.BlockSpec(memory_space=pltpu.VMEM),
        compiler_params=params(4),
        cost_estimate=pl.CostEstimate(flops=4 * QUARTER * D, bytes_accessed=2 * MIB, transcendentals=0),
        name="total",
    )(own, *others)


def owner_kernel(parts, out):
    total = parts[0].astype(jnp.float32)
    for k in range(1, parts.shape[0]):
        total = total + parts[k].astype(jnp.float32)
    update = quantized(total).astype(jnp.bfloat16)
    for k in range(out.shape[0]):
        out[k] = update


def owner_update(parts):
    return pl.pallas_call(
        owner_kernel,
        out_shape=jax.ShapeDtypeStruct((16, OWNED, BLOCK), jnp.bfloat16),
        in_specs=[pl.BlockSpec(memory_space=pltpu.VMEM)],
        out_specs=pl.BlockSpec(memory_space=pltpu.VMEM),
        compiler_params=params(8),
        cost_estimate=pl.CostEstimate(
            flops=parts.size, bytes_accessed=2 * MIB, transcendentals=0
        ),
        name="owner",
    )(parts)


def widen_kernel(count, *refs):
    indices, parts = refs[:count], refs[count : 2 * count]
    out, wide, sem = refs[-3:]
    rows = QUARTER // WSTEPS

    def copy(n, i):
        start = indices[n][0] * QUARTER + i * rows
        return pltpu.make_async_copy(
            wide.at[n, pl.ds(i * rows, rows), :],
            out.at[pl.ds(pl.multiple_of(start, 8), rows), :],
            sem.at[n, i],
        )

    for n, part in enumerate(parts):
        for i in range(WSTEPS):
            for r in range(i * rows // 8, (i + 1) * rows // 8):
                for b in range(COLS):
                    wide[n, r * 8 : r * 8 + 8, b * BLOCK : (b + 1) * BLOCK] = part[
                        r * COLS + b
                    ].astype(jnp.float32)
            copy(n, i).start()
    for n in range(count):
        for i in range(WSTEPS):
            copy(n, i).wait()


def widen(indices, parts, base):
    count = len(parts)
    smem, vmem = pl.BlockSpec(memory_space=pltpu.SMEM), pl.BlockSpec(memory_space=pltpu.VMEM)
    specs = [smem] * count + [vmem] * count
    args = [*indices, *parts]
    aliases = {}
    if base is not None:
        specs.append(pl.BlockSpec(memory_space=pltpu.HBM))
        args.append(base)
        aliases = {2 * count: 0}
    return pl.pallas_call(
        functools.partial(widen_kernel, count),
        out_shape=pltpu.HBM((D, D), jnp.float32),
        in_specs=specs,
        out_specs=pl.BlockSpec(memory_space=pltpu.HBM),
        scratch_shapes=[
            pltpu.VMEM((count, QUARTER, D), jnp.float32),
            pltpu.SemaphoreType.DMA((count, WSTEPS)),
        ],
        input_output_aliases=aliases,
        compiler_params=params(4),
        cost_estimate=pl.CostEstimate(flops=1 << 30, bytes_accessed=MIB, transcendentals=0),
        name="widen",
    )(*args)


def swap_cores(value):
    return lax.ppermute(value, "c", [(0, 1), (1, 0)])


def one(value):
    return value.astype(jnp.int32).reshape(1)


def on_device(activations, cotangent, carried_error, owner_error):
    core = lax.axis_index("c")
    x, y = lax.axis_index("x"), lax.axis_index("y")
    lead = jnp.where(core == 0, x, y)
    other_lead = x + y - lead
    spot = one(lax.axis_index(AXES) * owner_error.shape[0])
    error = carried_error.reshape(D, D)
    args = (activations, cotangent, error, owner_error)
    args = [pltpu.with_memory_space_constraint(v, pltpu.HBM) for v in args]
    v = gradient(spot, *args)
    sent = pick(one(1 - core), one(other_lead), v)
    got = {}
    for k in ORDER:
        got[k] = swap_cores(sent[k])
    arrived = []
    for k in ORDER:
        piece = pair(one(core), one(lead), v, got[k], k)
        if k:
            piece = lax.ppermute(piece, AXES, to_ahead(k))
        arrived.append(piece)
    parts = total_of(*arrived[::-1]).reshape(16, OWNED, BLOCK)
    parts = lax.all_to_all(parts, AXES, 0, 0, axis_index_groups=SIXTEENS, tiled=True)
    update = owner_update(parts)
    mine = lax.all_to_all(update, AXES, 0, 0, axis_index_groups=SIXTEENS, tiled=True)
    pieces = {0: mine.reshape(16 * PER_CHIP, 8, BLOCK)[:TILES]}
    for k in (1, 3, 2):
        pieces[k] = lax.ppermute(pieces[0], AXES, from_ahead(k))
    theirs = {}
    for k in (0, 1, 3, 2):
        theirs[k] = swap_cores(pieces[k])
    out = None
    for parts in WRITES.values():
        indices = [
            one(piece_index(core, (lead + k) % 4))
            if own
            else one(piece_index(1 - core, (other_lead + k) % 4))
            for k, own in parts
        ]
        parts = [pieces[k] if own else theirs[k] for k, own in parts]
        out = widen(indices, parts, out)
    return out


def solution(mesh):
    fine = Mesh(mesh.devices.reshape(SIZES), AXES)
    return jax.shard_map(
        on_device,
        mesh=fine,
        in_specs=(P(AXES, None), P(AXES, None), P(AXES, None, None), P(AXES, None)),
        out_specs=P(),
        check_vma=False,
    )
```

```python
import functools

import jax
import jax.numpy as jnp
import numpy as np
from jax import lax
from jax.experimental import pallas as pl
from jax.experimental.pallas import tpu as pltpu
from jax.sharding import Mesh
from jax.sharding import PartitionSpec as P


D = 1280
BLOCK = 128
HALF = D // 2
COLS = D // BLOCK
AXES = ("zl", "c", "zh", "y", "x")
SIZES = (2, 2, 2, 4, 4)
QUARTER = HALF // 4
TILES = QUARTER // 8 * COLS
PER_CHIP = -(-TILES // 16)
OWNED = PER_CHIP * 8
CHUNK = 512
MROWS = 256
EARLY = 3
WSTEPS = 5
MIB = 1 << 20
GRANT = 34
ORDER = (1, 3, 2, 0)
WRITES = {
    "write_0": ((0, True), (0, False)),
    "write_1": ((1, True), (1, False)),
    "write_2": ((3, True), (2, True)),
    "write_3": ((3, False), (2, False)),
}


def device(zl, c, zh, y, x):
    return int(np.ravel_multi_index((zl, c, zh, y, x), SIZES))


def line(core, lead):
    spots = [(zl, zh, o) for zl in range(2) for zh in range(2) for o in range(4)]
    if core == 0:
        return [device(zl, 0, zh, o, lead) for zl, zh, o in spots]
    return [device(zl, 1, zh, lead, o) for zl, zh, o in spots]


SIXTEENS = [line(core, lead) for core in range(2) for lead in range(4)]


def from_ahead(k):
    pairs = []
    for core in range(2):
        for lead in range(4):
            pairs += list(zip(line(core, lead ^ k), line(core, lead)))
    return pairs


def to_ahead(k):
    return [(source, target) for target, source in from_ahead(k)]


def params(mib, **more):
    return pltpu.CompilerParams(vmem_limit_bytes=mib * MIB, **more)


def quantized(v):
    largest = jnp.max(jnp.abs(v), axis=-1, keepdims=True)
    scale = ((largest + 1e-06) / 127.0).astype(jnp.bfloat16).astype(jnp.float32)
    level = (v * (1.0 / scale)).astype(jnp.bfloat16).astype(jnp.float32)
    return level * scale


def piece_start(core, quarter):
    return quarter // 2 * HALF + core * (HALF // 2) + quarter % 2 * QUARTER


def piece_index(core, quarter):
    return quarter // 2 * 4 + core * 2 + quarter % 2


def multiplied(a, c):
    return lax.dot_general(a, c, (((0,), (0,)), ((), ())), preferred_element_type=jnp.float32)


def gradient_kernel(
    spot, act, cot, error, owner, v, early_v, late_v, cot_v, err, own, acc, early_sem, late_sem, cot_sem, err_sem, own_sem
):
    chunks = cot.shape[0] // CHUNK
    blocks = D // MROWS

    def slab(i):
        return pl.ds(i * CHUNK, CHUNK)

    def early(i):
        return (
            pltpu.make_async_copy(
                act.at[slab(i), pl.ds(0, EARLY * MROWS)], early_v.at[slab(i), :], early_sem.at[i]
            ),
            pltpu.make_async_copy(cot.at[slab(i), :], cot_v.at[slab(i), :], cot_sem.at[i]),
        )

    def late(j):
        return pltpu.make_async_copy(
            act.at[:, pl.ds(j * MROWS, MROWS)], late_v.at[j - EARLY], late_sem.at[j - EARLY]
        )

    def load_err(j):
        at = pl.ds(j * MROWS, MROWS)
        return pltpu.make_async_copy(error.at[at, :], err.at[at, :], err_sem.at[j])

    def finish(j):
        at = slice(j * MROWS, (j + 1) * MROWS)
        for b in range(0, D, BLOCK):
            cols = slice(b, b + BLOCK)
            v[at, cols] = quantized(acc[at, cols] + err[at, cols])

    load_own = pltpu.make_async_copy(owner, own, own_sem)
    for i in range(2):
        for copy in early(i):
            copy.start()
    for i in range(chunks):
        for copy in early(i):
            copy.wait()
        if i + 2 < chunks:
            for copy in early(i + 2):
                copy.start()
        elif i + 2 == chunks:
            late(EARLY).start()
            for j in range(blocks):
                load_err(j).start()
                if EARLY < j + EARLY + 1 < blocks:
                    late(j + EARLY + 1).start()
            load_own.start()
        for j in range(EARLY):
            at = slice(j * MROWS, (j + 1) * MROWS)
            product = multiplied(early_v[i * CHUNK : (i + 1) * CHUNK, at], cot_v[i * CHUNK : (i + 1) * CHUNK, :])
            acc[at, :] = product if i == 0 else acc[at, :] + product
    done = 0
    for j in range(EARLY, blocks):
        late(j).wait()
        ready = j if j + 1 == blocks else min(j, done + 2 if j > EARLY else 1)
        for q in range(done, ready):
            load_err(q).wait()
        acc[j * MROWS : (j + 1) * MROWS, :] = multiplied(late_v[j - EARLY], cot_v[...])
        for q in range(done, ready):
            finish(q)
        done = ready
    load_own.wait()
    for q in range(done, blocks):
        load_err(q).wait()
        finish(q)
    row = spot[0]
    for shift in (0, 2, 4, 6):

        @pl.when(row % 8 == shift)
        def _():
            for i in range(2):
                low, high = max(shift - 8 * i, 0), min(shift + 10 - 8 * i, 8)
                rows = pl.ds(pl.multiple_of(row // 8 * 8 + 8 * i, 8), 8)
                mine = own[low - shift + 8 * i : high - shift + 8 * i, :]
                v[rows, :] = v[rows, :] + jnp.pad(mine, ((low, 8 - high), (0, 0)))


def gradient(spot, act, cot, error, owner):
    tokens = act.shape[0]
    hbm, vmem = pl.BlockSpec(memory_space=pltpu.HBM), pl.BlockSpec(memory_space=pltpu.VMEM)
    blocks, chunks = D // MROWS, tokens // CHUNK
    return pl.pallas_call(
        gradient_kernel,
        out_shape=pltpu.VMEM((D, D), jnp.float32),
        in_specs=[pl.BlockSpec(memory_space=pltpu.SMEM)] + [hbm] * 4,
        out_specs=vmem,
        scratch_shapes=[
            pltpu.VMEM((tokens, EARLY * MROWS), jnp.bfloat16),
            pltpu.VMEM((blocks - EARLY, tokens, MROWS), jnp.bfloat16),
            pltpu.VMEM((tokens, D), jnp.bfloat16),
            pltpu.VMEM((D, D), jnp.float32),
            pltpu.VMEM(owner.shape, jnp.float32),
            pltpu.VMEM((D, D), jnp.float32),
            pltpu.SemaphoreType.DMA((chunks,)),
            pltpu.SemaphoreType.DMA((blocks - EARLY,)),
            pltpu.SemaphoreType.DMA((chunks,)),
            pltpu.SemaphoreType.DMA((blocks,)),
            pltpu.SemaphoreType.DMA,
        ],
        compiler_params=params(GRANT),
        cost_estimate=pl.CostEstimate(
            flops=2 * tokens * D * D, bytes_accessed=17 * MIB, transcendentals=0
        ),
        name="gradient",
    )(spot, act, cot, error, owner)


def multiplied(a, c):
    return lax.dot_general(a, c, (((0,), (0,)), ((), ())), preferred_element_type=jnp.float32)


def pick_kernel(core, lead, v, *outs):
    for k, out in enumerate(outs):
        start = piece_start(core[0], lead[0] ^ k)
        out[...] = v[pl.ds(pl.multiple_of(start, 32), QUARTER), :].astype(out.dtype)


def pick(core, lead, v):
    smem, vmem = pl.BlockSpec(memory_space=pltpu.SMEM), pl.BlockSpec(memory_space=pltpu.VMEM)
    return pl.pallas_call(
        pick_kernel,
        out_shape=[jax.ShapeDtypeStruct((QUARTER, D), jnp.bfloat16)] * 4,
        in_specs=[smem, smem, vmem],
        out_specs=[vmem] * 4,
        compiler_params=params(4),
        cost_estimate=pl.CostEstimate(flops=1 << 28, bytes_accessed=2 * MIB, transcendentals=0),
        name="pick",
    )(core, lead, v)


def pair_kernel(k, core, lead, v, got, out):
    start = piece_start(core[0], lead[0] ^ k)
    kept = v[pl.ds(pl.multiple_of(start, 32), QUARTER), :]
    out[...] = (kept + got[...].astype(jnp.float32)).astype(out.dtype)


def pair(core, lead, v, got, k):
    smem, vmem = pl.BlockSpec(memory_space=pltpu.SMEM), pl.BlockSpec(memory_space=pltpu.VMEM)
    return pl.pallas_call(
        functools.partial(pair_kernel, k),
        out_shape=jax.ShapeDtypeStruct((QUARTER, D), jnp.bfloat16 if k else jnp.float32),
        in_specs=[smem, smem, vmem, vmem],
        out_specs=vmem,
        compiler_params=params(4),
        cost_estimate=pl.CostEstimate(flops=1 << 28, bytes_accessed=2 * MIB, transcendentals=0),
    )(core, lead, v, got)


def total_kernel(own, *rest):
    out = rest[-1]
    for b in range(COLS):
        at = slice(b * BLOCK, (b + 1) * BLOCK)
        total = own[:, at]
        for got in rest[:-1]:
            total = total + got[:, at].astype(jnp.float32)
        total = total.astype(jnp.bfloat16).reshape(QUARTER // 8, 8, BLOCK)
        for r in range(QUARTER // 8):
            out[r * COLS + b] = total[r]
    out[TILES:] = jnp.zeros_like(out[TILES:])


def total_of(own, *others):
    return pl.pallas_call(
        total_kernel,
        out_shape=jax.ShapeDtypeStruct((16 * PER_CHIP, 8, BLOCK), jnp.bfloat16),
        in_specs=[pl.BlockSpec(memory_space=pltpu.VMEM)] * (1 + len(others)),
        out_specs=pl.BlockSpec(memory_space=pltpu.VMEM),
        compiler_params=params(4),
        cost_estimate=pl.CostEstimate(flops=4 * QUARTER * D, bytes_accessed=2 * MIB, transcendentals=0),
        name="total",
    )(own, *others)


def owner_kernel(parts, out):
    total = parts[0].astype(jnp.float32)
    for k in range(1, parts.shape[0]):
        total = total + parts[k].astype(jnp.float32)
    update = quantized(total).astype(jnp.bfloat16)
    for k in range(out.shape[0]):
        out[k] = update


def owner_update(parts):
    return pl.pallas_call(
        owner_kernel,
        out_shape=jax.ShapeDtypeStruct((16, OWNED, BLOCK), jnp.bfloat16),
        in_specs=[pl.BlockSpec(memory_space=pltpu.VMEM)],
        out_specs=pl.BlockSpec(memory_space=pltpu.VMEM),
        compiler_params=params(8),
        cost_estimate=pl.CostEstimate(
            flops=parts.size, bytes_accessed=2 * MIB, transcendentals=0
        ),
        name="owner",
    )(parts)


def widen_kernel(count, *refs):
    indices, parts = refs[:count], refs[count : 2 * count]
    out, wide, sem = refs[-3:]
    rows = QUARTER // WSTEPS

    def copy(n, i):
        start = indices[n][0] * QUARTER + i * rows
        return pltpu.make_async_copy(
            wide.at[n, pl.ds(i * rows, rows), :],
            out.at[pl.ds(pl.multiple_of(start, 8), rows), :],
            sem.at[n, i],
        )

    for n, part in enumerate(parts):
        for i in range(WSTEPS):
            for r in range(i * rows // 8, (i + 1) * rows // 8):
                for b in range(COLS):
                    wide[n, r * 8 : r * 8 + 8, b * BLOCK : (b + 1) * BLOCK] = part[
                        r * COLS + b
                    ].astype(jnp.float32)
            copy(n, i).start()
    for n in range(count):
        for i in range(WSTEPS):
            copy(n, i).wait()


def widen(indices, parts, base):
    count = len(parts)
    smem, vmem = pl.BlockSpec(memory_space=pltpu.SMEM), pl.BlockSpec(memory_space=pltpu.VMEM)
    specs = [smem] * count + [vmem] * count
    args = [*indices, *parts]
    aliases = {}
    if base is not None:
        specs.append(pl.BlockSpec(memory_space=pltpu.HBM))
        args.append(base)
        aliases = {2 * count: 0}
    return pl.pallas_call(
        functools.partial(widen_kernel, count),
        out_shape=pltpu.HBM((D, D), jnp.float32),
        in_specs=specs,
        out_specs=pl.BlockSpec(memory_space=pltpu.HBM),
        scratch_shapes=[
            pltpu.VMEM((count, QUARTER, D), jnp.float32),
            pltpu.SemaphoreType.DMA((count, WSTEPS)),
        ],
        input_output_aliases=aliases,
        compiler_params=params(4),
        cost_estimate=pl.CostEstimate(flops=1 << 30, bytes_accessed=MIB, transcendentals=0),
        name="widen",
    )(*args)


def swap_cores(value):
    return lax.ppermute(value, "c", [(0, 1), (1, 0)])


def one(value):
    return value.astype(jnp.int32).reshape(1)


def on_device(activations, cotangent, carried_error, owner_error):
    core = lax.axis_index("c")
    x, y = lax.axis_index("x"), lax.axis_index("y")
    lead = jnp.where(core == 0, x, y)
    other_lead = x + y - lead
    spot = one(lax.axis_index(AXES) * owner_error.shape[0])
    error = carried_error.reshape(D, D)
    args = (activations, cotangent, error, owner_error)
    args = [pltpu.with_memory_space_constraint(v, pltpu.HBM) for v in args]
    v = gradient(spot, *args)
    sent = pick(one(1 - core), one(other_lead), v)
    got = {}
    for k in ORDER:
        got[k] = swap_cores(sent[k])
    arrived = []
    for k in ORDER:
        piece = pair(one(core), one(lead), v, got[k], k)
        if k:
            piece = lax.ppermute(piece, AXES, to_ahead(k))
        arrived.append(piece)
    parts = total_of(*arrived[::-1]).reshape(16, OWNED, BLOCK)
    parts = lax.all_to_all(parts, AXES, 0, 0, axis_index_groups=SIXTEENS, tiled=True)
    update = owner_update(parts)
    mine = lax.all_to_all(update, AXES, 0, 0, axis_index_groups=SIXTEENS, tiled=True)
    pieces = {0: mine.reshape(16 * PER_CHIP, 8, BLOCK)[:TILES]}
    for k in (1, 3, 2):
        pieces[k] = lax.ppermute(pieces[0], AXES, from_ahead(k))
    theirs = {}
    for k in (0, 1, 3, 2):
        theirs[k] = swap_cores(pieces[k])
    out = None
    for parts in WRITES.values():
        indices = [
            one(piece_index(core, lead ^ k))
            if own
            else one(piece_index(1 - core, other_lead ^ k))
            for k, own in parts
        ]
        parts = [pieces[k] if own else theirs[k] for k, own in parts]
        out = widen(indices, parts, out)
    return out


def solution(mesh):
    fine = Mesh(mesh.devices.reshape(SIZES), AXES)
    return jax.shard_map(
        on_device,
        mesh=fine,
        in_specs=(P(AXES, None), P(AXES, None), P(AXES, None, None), P(AXES, None)),
        out_specs=P(),
        check_vma=False,
    )
```

```python
import functools

import jax
import jax.numpy as jnp
import numpy as np
from jax import lax
from jax.experimental import pallas as pl
from jax.experimental.pallas import tpu as pltpu
from jax.sharding import Mesh
from jax.sharding import PartitionSpec as P


D = 1280
BLOCK = 128
HALF = D // 2
COLS = D // BLOCK
AXES = ("zl", "c", "zh", "y", "x")
SIZES = (2, 2, 2, 4, 4)
QUARTER = HALF // 4
TILES = QUARTER // 8 * COLS
PER_CHIP = -(-TILES // 16)
OWNED = PER_CHIP * 8
CHUNK = 512
MROWS = 256
EARLY = 4
AHEAD = 3
WSTEPS = 2
MIB = 1 << 20
GRANT = 34
ORDER = (1, 3, 2, 0)
WRITES = {
    "write_0": ((0, True), (0, False)),
    "write_1": ((1, True), (1, False)),
    "write_2": ((3, True), (2, True)),
    "write_3": ((3, False), (2, False)),
}


def device(zl, c, zh, y, x):
    return int(np.ravel_multi_index((zl, c, zh, y, x), SIZES))


def line(core, lead):
    spots = [(zl, zh, o) for zl in range(2) for zh in range(2) for o in range(4)]
    if core == 0:
        return [device(zl, 0, zh, o, lead) for zl, zh, o in spots]
    return [device(zl, 1, zh, lead, o) for zl, zh, o in spots]


SIXTEENS = [line(core, lead) for core in range(2) for lead in range(4)]


def from_ahead(k):
    pairs = []
    for core in range(2):
        for lead in range(4):
            pairs += list(zip(line(core, lead ^ k), line(core, lead)))
    return pairs


def to_ahead(k):
    return [(source, target) for target, source in from_ahead(k)]


def params(mib, **more):
    return pltpu.CompilerParams(vmem_limit_bytes=mib * MIB, **more)


def quantized(v):
    largest = jnp.max(jnp.abs(v), axis=-1, keepdims=True)
    scale = ((largest + 1e-06) / 127.0).astype(jnp.bfloat16).astype(jnp.float32)
    level = (v * (1.0 / scale)).astype(jnp.bfloat16).astype(jnp.float32)
    return level * scale


def piece_start(core, quarter):
    return quarter // 2 * HALF + core * (HALF // 2) + quarter % 2 * QUARTER


def piece_index(core, quarter):
    return quarter // 2 * 4 + core * 2 + quarter % 2


def multiplied(a, c):
    return lax.dot_general(a, c, (((0,), (0,)), ((), ())), preferred_element_type=jnp.float32)


def gradient_kernel(
    spot, act, cot, error, owner, v, early_v, late_v, cot_v, err, own, acc, early_sem, late_sem, cot_sem, err_sem, own_sem
):
    chunks = cot.shape[0] // CHUNK
    blocks = D // MROWS

    def slab(i):
        return pl.ds(i * CHUNK, CHUNK)

    def early(i):
        return (
            pltpu.make_async_copy(
                act.at[slab(i), pl.ds(0, EARLY * MROWS)], early_v.at[slab(i), :], early_sem.at[i]
            ),
            pltpu.make_async_copy(cot.at[slab(i), :], cot_v.at[slab(i), :], cot_sem.at[i]),
        )

    def late(j):
        return pltpu.make_async_copy(
            act.at[:, pl.ds(j * MROWS, MROWS)], late_v.at[j - EARLY], late_sem.at[j - EARLY]
        )

    def load_err(j):
        at = pl.ds(j * MROWS, MROWS)
        return pltpu.make_async_copy(error.at[at, :], err.at[at, :], err_sem.at[j])

    def finish(j):
        at = slice(j * MROWS, (j + 1) * MROWS)
        for b in range(0, D, BLOCK):
            cols = slice(b, b + BLOCK)
            v[at, cols] = quantized(acc[at, cols] + err[at, cols])

    load_own = pltpu.make_async_copy(owner, own, own_sem)
    for i in range(AHEAD):
        for copy in early(i):
            copy.start()
    for i in range(chunks):
        for copy in early(i):
            copy.wait()
        if i + AHEAD < chunks:
            for copy in early(i + AHEAD):
                copy.start()
        elif i + AHEAD == chunks:
            late(EARLY).start()
            for j in range(blocks):
                load_err(j).start()
                if EARLY < j + EARLY + 1 < blocks:
                    late(j + EARLY + 1).start()
            load_own.start()
        for j in range(EARLY):
            at = slice(j * MROWS, (j + 1) * MROWS)
            product = multiplied(early_v[i * CHUNK : (i + 1) * CHUNK, at], cot_v[i * CHUNK : (i + 1) * CHUNK, :])
            acc[at, :] = product if i == 0 else acc[at, :] + product
    done = 0
    for j in range(EARLY, blocks):
        late(j).wait()
        ready = j if j + 1 == blocks else min(j, done + 2 if j > EARLY else 1)
        for q in range(done, ready):
            load_err(q).wait()
        acc[j * MROWS : (j + 1) * MROWS, :] = multiplied(late_v[j - EARLY], cot_v[...])
        for q in range(done, ready):
            finish(q)
        done = ready
    load_own.wait()
    for q in range(done, blocks):
        load_err(q).wait()
        finish(q)
    row = spot[0]
    for shift in (0, 2, 4, 6):

        @pl.when(row % 8 == shift)
        def _():
            for i in range(2):
                low, high = max(shift - 8 * i, 0), min(shift + 10 - 8 * i, 8)
                rows = pl.ds(pl.multiple_of(row // 8 * 8 + 8 * i, 8), 8)
                mine = own[low - shift + 8 * i : high - shift + 8 * i, :]
                v[rows, :] = v[rows, :] + jnp.pad(mine, ((low, 8 - high), (0, 0)))


def gradient(spot, act, cot, error, owner):
    tokens = act.shape[0]
    hbm, vmem = pl.BlockSpec(memory_space=pltpu.HBM), pl.BlockSpec(memory_space=pltpu.VMEM)
    blocks, chunks = D // MROWS, tokens // CHUNK
    return pl.pallas_call(
        gradient_kernel,
        out_shape=pltpu.VMEM((D, D), jnp.float32),
        in_specs=[pl.BlockSpec(memory_space=pltpu.SMEM)] + [hbm] * 4,
        out_specs=vmem,
        scratch_shapes=[
            pltpu.VMEM((tokens, EARLY * MROWS), jnp.bfloat16),
            pltpu.VMEM((blocks - EARLY, tokens, MROWS), jnp.bfloat16),
            pltpu.VMEM((tokens, D), jnp.bfloat16),
            pltpu.VMEM((D, D), jnp.float32),
            pltpu.VMEM(owner.shape, jnp.float32),
            pltpu.VMEM((D, D), jnp.float32),
            pltpu.SemaphoreType.DMA((chunks,)),
            pltpu.SemaphoreType.DMA((blocks - EARLY,)),
            pltpu.SemaphoreType.DMA((chunks,)),
            pltpu.SemaphoreType.DMA((blocks,)),
            pltpu.SemaphoreType.DMA,
        ],
        compiler_params=params(GRANT),
        cost_estimate=pl.CostEstimate(
            flops=2 * tokens * D * D, bytes_accessed=17 * MIB, transcendentals=0
        ),
        name="gradient",
    )(spot, act, cot, error, owner)


def multiplied(a, c):
    return lax.dot_general(a, c, (((0,), (0,)), ((), ())), preferred_element_type=jnp.float32)


def pick_kernel(core, lead, v, *outs):
    for k, out in enumerate(outs):
        start = piece_start(core[0], lead[0] ^ k)
        out[...] = v[pl.ds(pl.multiple_of(start, 32), QUARTER), :].astype(out.dtype)


def pick(core, lead, v):
    smem, vmem = pl.BlockSpec(memory_space=pltpu.SMEM), pl.BlockSpec(memory_space=pltpu.VMEM)
    return pl.pallas_call(
        pick_kernel,
        out_shape=[jax.ShapeDtypeStruct((QUARTER, D), jnp.bfloat16)] * 4,
        in_specs=[smem, smem, vmem],
        out_specs=[vmem] * 4,
        compiler_params=params(4),
        cost_estimate=pl.CostEstimate(flops=1 << 28, bytes_accessed=2 * MIB, transcendentals=0),
        name="pick",
    )(core, lead, v)


def pair_kernel(k, core, lead, v, got, out):
    start = piece_start(core[0], lead[0] ^ k)
    kept = v[pl.ds(pl.multiple_of(start, 32), QUARTER), :]
    out[...] = (kept + got[...].astype(jnp.float32)).astype(out.dtype)


def pair(core, lead, v, got, k):
    smem, vmem = pl.BlockSpec(memory_space=pltpu.SMEM), pl.BlockSpec(memory_space=pltpu.VMEM)
    return pl.pallas_call(
        functools.partial(pair_kernel, k),
        out_shape=jax.ShapeDtypeStruct((QUARTER, D), jnp.bfloat16 if k else jnp.float32),
        in_specs=[smem, smem, vmem, vmem],
        out_specs=vmem,
        compiler_params=params(4),
        cost_estimate=pl.CostEstimate(flops=1 << 28, bytes_accessed=2 * MIB, transcendentals=0),
    )(core, lead, v, got)


def total_kernel(own, *rest):
    out = rest[-1]
    for b in range(COLS):
        at = slice(b * BLOCK, (b + 1) * BLOCK)
        total = own[:, at]
        for got in rest[:-1]:
            total = total + got[:, at].astype(jnp.float32)
        total = total.astype(jnp.bfloat16).reshape(QUARTER // 8, 8, BLOCK)
        for r in range(QUARTER // 8):
            out[r * COLS + b] = total[r]
    out[TILES:] = jnp.zeros_like(out[TILES:])


def total_of(own, *others):
    return pl.pallas_call(
        total_kernel,
        out_shape=jax.ShapeDtypeStruct((16 * PER_CHIP, 8, BLOCK), jnp.bfloat16),
        in_specs=[pl.BlockSpec(memory_space=pltpu.VMEM)] * (1 + len(others)),
        out_specs=pl.BlockSpec(memory_space=pltpu.VMEM),
        compiler_params=params(4),
        cost_estimate=pl.CostEstimate(flops=4 * QUARTER * D, bytes_accessed=2 * MIB, transcendentals=0),
        name="total",
    )(own, *others)


def owner_kernel(parts, out):
    total = parts[0].astype(jnp.float32)
    for k in range(1, parts.shape[0]):
        total = total + parts[k].astype(jnp.float32)
    update = quantized(total).astype(jnp.bfloat16)
    for k in range(out.shape[0]):
        out[k] = update


def owner_update(parts):
    return pl.pallas_call(
        owner_kernel,
        out_shape=jax.ShapeDtypeStruct((16, OWNED, BLOCK), jnp.bfloat16),
        in_specs=[pl.BlockSpec(memory_space=pltpu.VMEM)],
        out_specs=pl.BlockSpec(memory_space=pltpu.VMEM),
        compiler_params=params(8),
        cost_estimate=pl.CostEstimate(
            flops=parts.size, bytes_accessed=2 * MIB, transcendentals=0
        ),
        name="owner",
    )(parts)


def widen_kernel(count, *refs):
    indices, parts = refs[:count], refs[count : 2 * count]
    out, wide, sem = refs[-3:]
    rows = QUARTER // WSTEPS

    def copy(n, i):
        start = indices[n][0] * QUARTER + i * rows
        return pltpu.make_async_copy(
            wide.at[n, pl.ds(i * rows, rows), :],
            out.at[pl.ds(pl.multiple_of(start, 8), rows), :],
            sem.at[n, i],
        )

    for n, part in enumerate(parts):
        for i in range(WSTEPS):
            for r in range(i * rows // 8, (i + 1) * rows // 8):
                for b in range(COLS):
                    wide[n, r * 8 : r * 8 + 8, b * BLOCK : (b + 1) * BLOCK] = part[
                        r * COLS + b
                    ].astype(jnp.float32)
            copy(n, i).start()
    for n in range(count):
        for i in range(WSTEPS):
            copy(n, i).wait()


def widen(indices, parts, base):
    count = len(parts)
    smem, vmem = pl.BlockSpec(memory_space=pltpu.SMEM), pl.BlockSpec(memory_space=pltpu.VMEM)
    specs = [smem] * count + [vmem] * count
    args = [*indices, *parts]
    aliases = {}
    if base is not None:
        specs.append(pl.BlockSpec(memory_space=pltpu.HBM))
        args.append(base)
        aliases = {2 * count: 0}
    return pl.pallas_call(
        functools.partial(widen_kernel, count),
        out_shape=pltpu.HBM((D, D), jnp.float32),
        in_specs=specs,
        out_specs=pl.BlockSpec(memory_space=pltpu.HBM),
        scratch_shapes=[
            pltpu.VMEM((count, QUARTER, D), jnp.float32),
            pltpu.SemaphoreType.DMA((count, WSTEPS)),
        ],
        input_output_aliases=aliases,
        compiler_params=params(4),
        cost_estimate=pl.CostEstimate(flops=1 << 30, bytes_accessed=MIB, transcendentals=0),
        name="widen",
    )(*args)


def swap_cores(value):
    return lax.ppermute(value, "c", [(0, 1), (1, 0)])


def one(value):
    return value.astype(jnp.int32).reshape(1)


def on_device(activations, cotangent, carried_error, owner_error):
    core = lax.axis_index("c")
    x, y = lax.axis_index("x"), lax.axis_index("y")
    lead = jnp.where(core == 0, x, y)
    other_lead = x + y - lead
    spot = one(lax.axis_index(AXES) * owner_error.shape[0])
    error = carried_error.reshape(D, D)
    args = (activations, cotangent, error, owner_error)
    args = [pltpu.with_memory_space_constraint(v, pltpu.HBM) for v in args]
    v = gradient(spot, *args)
    sent = pick(one(1 - core), one(other_lead), v)
    got = {}
    for k in ORDER:
        got[k] = swap_cores(sent[k])
    arrived = []
    for k in ORDER:
        piece = pair(one(core), one(lead), v, got[k], k)
        if k:
            piece = lax.ppermute(piece, AXES, to_ahead(k))
        arrived.append(piece)
    parts = total_of(*arrived[::-1]).reshape(16, OWNED, BLOCK)
    parts = lax.all_to_all(parts, AXES, 0, 0, axis_index_groups=SIXTEENS, tiled=True)
    update = owner_update(parts)
    mine = lax.all_to_all(update, AXES, 0, 0, axis_index_groups=SIXTEENS, tiled=True)
    pieces = {0: mine.reshape(16 * PER_CHIP, 8, BLOCK)[:TILES]}
    for k in (1, 3, 2):
        pieces[k] = lax.ppermute(pieces[0], AXES, from_ahead(k))
    theirs = {}
    for k in (0, 1, 3, 2):
        theirs[k] = swap_cores(pieces[k])
    out = None
    for parts in WRITES.values():
        indices = [
            one(piece_index(core, lead ^ k))
            if own
            else one(piece_index(1 - core, other_lead ^ k))
            for k, own in parts
        ]
        parts = [pieces[k] if own else theirs[k] for k, own in parts]
        out = widen(indices, parts, out)
    return out


def solution(mesh):
    fine = Mesh(mesh.devices.reshape(SIZES), AXES)
    return jax.shard_map(
        on_device,
        mesh=fine,
        in_specs=(P(AXES, None), P(AXES, None), P(AXES, None, None), P(AXES, None)),
        out_specs=P(),
        check_vma=False,
    )
```

```python
import functools

import jax
import jax.numpy as jnp
import numpy as np
from jax import lax
from jax.experimental import pallas as pl
from jax.experimental.pallas import tpu as pltpu
from jax.sharding import Mesh
from jax.sharding import PartitionSpec as P


D = 1280
BLOCK = 128
HALF = D // 2
COLS = D // BLOCK
AXES = ("zl", "c", "zh", "y", "x")
SIZES = (2, 2, 2, 4, 4)
QUARTER = HALF // 4
TILES = QUARTER // 8 * COLS
PER_CHIP = -(-TILES // 16)
OWNED = PER_CHIP * 8
CHUNK = 512
MROWS = 256
EARLY = 4
AHEAD = 3
WSTEPS = 2
MIB = 1 << 20
GRANT = 34
ORDER = (1, 3, 2, 0)
WRITES = {
    "write_0": ((0, True), (0, False)),
    "write_1": ((1, True), (1, False)),
    "write_2": ((3, True), (2, True)),
    "write_3": ((3, False), (2, False)),
}


def device(zl, c, zh, y, x):
    return int(np.ravel_multi_index((zl, c, zh, y, x), SIZES))


def line(core, lead):
    spots = [(zl, zh, o) for zl in range(2) for zh in range(2) for o in range(4)]
    if core == 0:
        return [device(zl, 0, zh, o, lead) for zl, zh, o in spots]
    return [device(zl, 1, zh, lead, o) for zl, zh, o in spots]


SIXTEENS = [line(core, lead) for core in range(2) for lead in range(4)]


def from_ahead(k):
    pairs = []
    for core in range(2):
        for lead in range(4):
            pairs += list(zip(line(core, lead ^ k), line(core, lead)))
    return pairs


def to_ahead(k):
    return [(source, target) for target, source in from_ahead(k)]


def params(mib, **more):
    return pltpu.CompilerParams(vmem_limit_bytes=mib * MIB, **more)


def quantized(v):
    largest = jnp.max(jnp.abs(v), axis=-1, keepdims=True)
    scale = ((largest + 1e-06) / 127.0).astype(jnp.bfloat16).astype(jnp.float32)
    level = (v * (1.0 / scale)).astype(jnp.bfloat16).astype(jnp.float32)
    return level * scale


def piece_start(core, quarter):
    return quarter // 2 * HALF + core * (HALF // 2) + quarter % 2 * QUARTER


def piece_index(core, quarter):
    return quarter // 2 * 4 + core * 2 + quarter % 2


def multiplied(a, c):
    return lax.dot_general(a, c, (((0,), (0,)), ((), ())), preferred_element_type=jnp.float32)


def gradient_kernel(
    core, lead, spot, act, cot, error, owner, v, s0, s1, s2, s3, early_v, late_v, cot_v, err, own, acc, early_sem, late_sem, cot_sem, err_sem, own_sem
):
    chunks = cot.shape[0] // CHUNK
    blocks = D // MROWS

    def slab(i):
        return pl.ds(i * CHUNK, CHUNK)

    def early(i):
        return (
            pltpu.make_async_copy(
                act.at[slab(i), pl.ds(0, EARLY * MROWS)], early_v.at[slab(i), :], early_sem.at[i]
            ),
            pltpu.make_async_copy(cot.at[slab(i), :], cot_v.at[slab(i), :], cot_sem.at[i]),
        )

    def late(j):
        return pltpu.make_async_copy(
            act.at[:, pl.ds(j * MROWS, MROWS)], late_v.at[j - EARLY], late_sem.at[j - EARLY]
        )

    def load_err(j):
        at = pl.ds(j * MROWS, MROWS)
        return pltpu.make_async_copy(error.at[at, :], err.at[at, :], err_sem.at[j])

    def finish(j):
        at = slice(j * MROWS, (j + 1) * MROWS)
        for b in range(0, D, BLOCK):
            cols = slice(b, b + BLOCK)
            v[at, cols] = quantized(acc[at, cols] + err[at, cols])

    load_own = pltpu.make_async_copy(owner, own, own_sem)
    for i in range(AHEAD):
        for copy in early(i):
            copy.start()
    for i in range(chunks):
        for copy in early(i):
            copy.wait()
        if i + AHEAD < chunks:
            for copy in early(i + AHEAD):
                copy.start()
        elif i + AHEAD == chunks:
            late(EARLY).start()
            for j in range(blocks):
                load_err(j).start()
                if EARLY < j + EARLY + 1 < blocks:
                    late(j + EARLY + 1).start()
            load_own.start()
        for j in range(EARLY):
            at = slice(j * MROWS, (j + 1) * MROWS)
            product = multiplied(early_v[i * CHUNK : (i + 1) * CHUNK, at], cot_v[i * CHUNK : (i + 1) * CHUNK, :])
            acc[at, :] = product if i == 0 else acc[at, :] + product
    done = 0
    for j in range(EARLY, blocks):
        late(j).wait()
        ready = j if j + 1 == blocks else min(j, done + 2 if j > EARLY else 1)
        for q in range(done, ready):
            load_err(q).wait()
        acc[j * MROWS : (j + 1) * MROWS, :] = multiplied(late_v[j - EARLY], cot_v[...])
        for q in range(done, ready):
            finish(q)
        done = ready
    load_own.wait()
    for q in range(done, blocks):
        load_err(q).wait()
        finish(q)
    row = spot[0]
    for shift in (0, 2, 4, 6):

        @pl.when(row % 8 == shift)
        def _():
            for i in range(2):
                low, high = max(shift - 8 * i, 0), min(shift + 10 - 8 * i, 8)
                rows = pl.ds(pl.multiple_of(row // 8 * 8 + 8 * i, 8), 8)
                mine = own[low - shift + 8 * i : high - shift + 8 * i, :]
                v[rows, :] = v[rows, :] + jnp.pad(mine, ((low, 8 - high), (0, 0)))
    for k, out in enumerate((s0, s1, s2, s3)):
        start = piece_start(core[0], lead[0] ^ k)
        out[...] = v[pl.ds(pl.multiple_of(start, 32), QUARTER), :].astype(out.dtype)


def gradient(core, lead, spot, act, cot, error, owner):
    tokens = act.shape[0]
    hbm, vmem = pl.BlockSpec(memory_space=pltpu.HBM), pl.BlockSpec(memory_space=pltpu.VMEM)
    blocks, chunks = D // MROWS, tokens // CHUNK
    return pl.pallas_call(
        gradient_kernel,
        out_shape=[pltpu.VMEM((D, D), jnp.float32)]
        + [jax.ShapeDtypeStruct((QUARTER, D), jnp.bfloat16)] * 4,
        in_specs=[pl.BlockSpec(memory_space=pltpu.SMEM)] * 3 + [hbm] * 4,
        out_specs=[vmem] * 5,
        scratch_shapes=[
            pltpu.VMEM((tokens, EARLY * MROWS), jnp.bfloat16),
            pltpu.VMEM((blocks - EARLY, tokens, MROWS), jnp.bfloat16),
            pltpu.VMEM((tokens, D), jnp.bfloat16),
            pltpu.VMEM((D, D), jnp.float32),
            pltpu.VMEM(owner.shape, jnp.float32),
            pltpu.VMEM((D, D), jnp.float32),
            pltpu.SemaphoreType.DMA((chunks,)),
            pltpu.SemaphoreType.DMA((blocks - EARLY,)),
            pltpu.SemaphoreType.DMA((chunks,)),
            pltpu.SemaphoreType.DMA((blocks,)),
            pltpu.SemaphoreType.DMA,
        ],
        compiler_params=params(GRANT),
        cost_estimate=pl.CostEstimate(
            flops=2 * tokens * D * D, bytes_accessed=17 * MIB, transcendentals=0
        ),
        name="gradient",
    )(core, lead, spot, act, cot, error, owner)


def multiplied(a, c):
    return lax.dot_general(a, c, (((0,), (0,)), ((), ())), preferred_element_type=jnp.float32)


def pair_kernel(k, core, lead, v, got, out):
    start = piece_start(core[0], lead[0] ^ k)
    kept = v[pl.ds(pl.multiple_of(start, 32), QUARTER), :]
    out[...] = (kept + got[...].astype(jnp.float32)).astype(out.dtype)


def pair(core, lead, v, got, k):
    smem, vmem = pl.BlockSpec(memory_space=pltpu.SMEM), pl.BlockSpec(memory_space=pltpu.VMEM)
    return pl.pallas_call(
        functools.partial(pair_kernel, k),
        out_shape=jax.ShapeDtypeStruct((QUARTER, D), jnp.bfloat16 if k else jnp.float32),
        in_specs=[smem, smem, vmem, vmem],
        out_specs=vmem,
        compiler_params=params(4),
        cost_estimate=pl.CostEstimate(flops=1 << 28, bytes_accessed=2 * MIB, transcendentals=0),
    )(core, lead, v, got)


def total_kernel(own, *rest):
    out = rest[-1]
    for b in range(COLS):
        at = slice(b * BLOCK, (b + 1) * BLOCK)
        total = own[:, at]
        for got in rest[:-1]:
            total = total + got[:, at].astype(jnp.float32)
        total = total.astype(jnp.bfloat16).reshape(QUARTER // 8, 8, BLOCK)
        for r in range(QUARTER // 8):
            out[r * COLS + b] = total[r]
    out[TILES:] = jnp.zeros_like(out[TILES:])


def total_of(own, *others):
    return pl.pallas_call(
        total_kernel,
        out_shape=jax.ShapeDtypeStruct((16 * PER_CHIP, 8, BLOCK), jnp.bfloat16),
        in_specs=[pl.BlockSpec(memory_space=pltpu.VMEM)] * (1 + len(others)),
        out_specs=pl.BlockSpec(memory_space=pltpu.VMEM),
        compiler_params=params(4),
        cost_estimate=pl.CostEstimate(flops=4 * QUARTER * D, bytes_accessed=2 * MIB, transcendentals=0),
        name="total",
    )(own, *others)


def owner_kernel(parts, out):
    total = parts[0].astype(jnp.float32)
    for k in range(1, parts.shape[0]):
        total = total + parts[k].astype(jnp.float32)
    update = quantized(total).astype(jnp.bfloat16)
    for k in range(out.shape[0]):
        out[k] = update


def owner_update(parts):
    return pl.pallas_call(
        owner_kernel,
        out_shape=jax.ShapeDtypeStruct((16, OWNED, BLOCK), jnp.bfloat16),
        in_specs=[pl.BlockSpec(memory_space=pltpu.VMEM)],
        out_specs=pl.BlockSpec(memory_space=pltpu.VMEM),
        compiler_params=params(8),
        cost_estimate=pl.CostEstimate(
            flops=parts.size, bytes_accessed=2 * MIB, transcendentals=0
        ),
        name="owner",
    )(parts)


def widen_kernel(count, *refs):
    indices, parts = refs[:count], refs[count : 2 * count]
    out, wide, sem = refs[-3:]
    rows = QUARTER // WSTEPS

    def copy(n, i):
        start = indices[n][0] * QUARTER + i * rows
        return pltpu.make_async_copy(
            wide.at[n, pl.ds(i * rows, rows), :],
            out.at[pl.ds(pl.multiple_of(start, 8), rows), :],
            sem.at[n, i],
        )

    for n, part in enumerate(parts):
        for i in range(WSTEPS):
            for r in range(i * rows // 8, (i + 1) * rows // 8):
                for b in range(COLS):
                    wide[n, r * 8 : r * 8 + 8, b * BLOCK : (b + 1) * BLOCK] = part[
                        r * COLS + b
                    ].astype(jnp.float32)
            copy(n, i).start()
    for n in range(count):
        for i in range(WSTEPS):
            copy(n, i).wait()


def widen(indices, parts, base):
    count = len(parts)
    smem, vmem = pl.BlockSpec(memory_space=pltpu.SMEM), pl.BlockSpec(memory_space=pltpu.VMEM)
    specs = [smem] * count + [vmem] * count
    args = [*indices, *parts]
    aliases = {}
    if base is not None:
        specs.append(pl.BlockSpec(memory_space=pltpu.HBM))
        args.append(base)
        aliases = {2 * count: 0}
    return pl.pallas_call(
        functools.partial(widen_kernel, count),
        out_shape=pltpu.HBM((D, D), jnp.float32),
        in_specs=specs,
        out_specs=pl.BlockSpec(memory_space=pltpu.HBM),
        scratch_shapes=[
            pltpu.VMEM((count, QUARTER, D), jnp.float32),
            pltpu.SemaphoreType.DMA((count, WSTEPS)),
        ],
        input_output_aliases=aliases,
        compiler_params=params(4),
        cost_estimate=pl.CostEstimate(flops=1 << 30, bytes_accessed=MIB, transcendentals=0),
        name="widen",
    )(*args)


def swap_cores(value):
    return lax.ppermute(value, "c", [(0, 1), (1, 0)])


def one(value):
    return value.astype(jnp.int32).reshape(1)


def on_device(activations, cotangent, carried_error, owner_error):
    core = lax.axis_index("c")
    x, y = lax.axis_index("x"), lax.axis_index("y")
    lead = jnp.where(core == 0, x, y)
    other_lead = x + y - lead
    spot = one(lax.axis_index(AXES) * owner_error.shape[0])
    error = carried_error.reshape(D, D)
    args = (activations, cotangent, error, owner_error)
    args = [pltpu.with_memory_space_constraint(v, pltpu.HBM) for v in args]
    v, *sent = gradient(one(1 - core), one(other_lead), spot, *args)
    got = {}
    for k in ORDER:
        got[k] = swap_cores(sent[k])
    arrived = []
    for k in ORDER:
        piece = pair(one(core), one(lead), v, got[k], k)
        if k:
            piece = lax.ppermute(piece, AXES, to_ahead(k))
        arrived.append(piece)
    parts = total_of(*arrived[::-1]).reshape(16, OWNED, BLOCK)
    parts = lax.all_to_all(parts, AXES, 0, 0, axis_index_groups=SIXTEENS, tiled=True)
    update = owner_update(parts)
    mine = lax.all_to_all(update, AXES, 0, 0, axis_index_groups=SIXTEENS, tiled=True)
    pieces = {0: mine.reshape(16 * PER_CHIP, 8, BLOCK)[:TILES]}
    for k in (1, 3, 2):
        pieces[k] = lax.ppermute(pieces[0], AXES, from_ahead(k))
    theirs = {}
    for k in (0, 1, 3, 2):
        theirs[k] = swap_cores(pieces[k])
    out = None
    for parts in WRITES.values():
        indices = [
            one(piece_index(core, lead ^ k))
            if own
            else one(piece_index(1 - core, other_lead ^ k))
            for k, own in parts
        ]
        parts = [pieces[k] if own else theirs[k] for k, own in parts]
        out = widen(indices, parts, out)
    return out


def solution(mesh):
    fine = Mesh(mesh.devices.reshape(SIZES), AXES)
    return jax.shard_map(
        on_device,
        mesh=fine,
        in_specs=(P(AXES, None), P(AXES, None), P(AXES, None, None), P(AXES, None)),
        out_specs=P(),
        check_vma=False,
    )
```
